32 devices in a mesh: blk: 2 (over y), uly: 4 (over x, core), dp: 4 (over z).
Axes of the slice: x: 2, y: 2, z: 4, core: 2. Of those that a mesh axis runs over, the one named last changes fastest.
Arguments:
- tokens: bfloat16 [1024, 4096], P(('uly', 'dp')), may hold values from -6 to 6
- expert_ids: int32 [1024, 8], P(('uly', 'dp')), may hold values from 0 to 15, all different within a row; in each aligned block of 64 rows (0 to 63, 64 to 127, ...) at most 40 rows name the same one
- route_weight: float32 [1024, 8], P(('uly', 'dp')), may hold values from 0.05 to 0.5
- w_gate: bfloat16 [16, 4096, 1024], P(('uly', 'dp'), None, 'blk'), may hold values from -0.09375 to 0.09375
- w_up: bfloat16 [16, 4096, 1024], P(('uly', 'dp'), None, 'blk'), may hold values from -0.09375 to 0.09375
- w_down: bfloat16 [16, 1024, 4096], P(('uly', 'dp'), 'blk'), may hold values from -0.1875 to 0.1875
Outputs:
- mixed: bfloat16 [1024, 4096], P(('uly', 'dp'), 'blk')
The draws below stay inside these ranges and needn't reach their ends.
Inputs may be any that keep to these rules, and one draw needn't show every extreme that they name: `expert_ids`: each row names 8 different experts. In each aligned block of 64 rows (the rows of one device) no expert is named by more than 40 rows, and in some block one expert is named by exactly 40 rows.
All inputs are finite; a program needn't handle non-finite values.
Results may differ from the reference program's by a relative error of at most 0.015.
Values may be sent and summed in bfloat16 or wider, within the bound.
A program may use at most 64 MiB of HBM per device.

```python
import math
import jax
import jax.numpy as jnp
import numpy as np
from jax import lax

D = 4096
FF = 1024
TOPK = 8
TOK_DEV = 64
EXPERTS = 16
CAP = 40
TOKENS = 1024
N_BLK = 2
N_ULY = 4
N_DP = 4


def levels(own_key, shape, shards, least, largest):
    def one(axis_at, shards_of):
        heights = jax.random.uniform(jax.random.fold_in(jax.random.fold_in(own_key, 6), axis_at), (shards_of,), jnp.float32, least / len(shards), largest / len(shards))
        return jnp.repeat(jnp.exp(heights), shape[axis_at] // shards_of).reshape((-1,) + (1,) * (len(shape) - axis_at - 1))

    gain = one(*shards[0])
    for cut in shards[1:]:
        gain = gain * one(*cut)
    return gain


def shared_out(own_key, own, number, rows, number_of, top, limit, skew):
    ranking = jax.random.permutation(own_key, number_of)
    crowded, usual = load_shares(number_of, rows * top, limit, skew, True), load_shares(number_of, rows * top, limit, skew, False)
    places = jnp.arange(number_of)

    def named(tallies, turn):
        used = int((tallies > 0).sum())
        fixed = max(1, used // 4)
        moved = fixed + (places - fixed + turn * (used - fixed)) % max(1, number_of - fixed)
        return jnp.zeros((number_of,), jnp.int32).at[ranking[jnp.where(places < fixed, places, moved)]].set(jnp.asarray(tallies, jnp.int32))

    tallies = jnp.where(number % 4 == 0, named(crowded, number // 4), named(usual, number - number // 4 - 1))
    mixed = jax.random.permutation(jax.random.fold_in(own, 3), number_of)
    source_of, receiver = mixed[0:number_of // 2 * 2:2], mixed[1:number_of // 2 * 2:2]
    slack = jnp.minimum(tallies[source_of] - 1, limit - tallies[receiver]) // 2
    slack = jnp.where((source_of == ranking[0]) | (receiver == ranking[0]) | (tallies[receiver] == 0), 0, jnp.maximum(slack, 0))
    moved = jax.random.randint(jax.random.fold_in(own, 4), (number_of // 2,), 0, 1 << 20) % (slack + 1)
    tallies = tallies.at[source_of].add(-moved).at[receiver].add(moved)
    items = jnp.searchsorted(jnp.cumsum(tallies), jnp.arange(rows * top), side="right").astype(jnp.int32)
    table = items.reshape(top, rows).T
    table = table[jax.random.permutation(jax.random.fold_in(own, 1), rows)]
    turn = jax.random.randint(jax.random.fold_in(own, 2), (rows, 1), 0, top)
    return jnp.take_along_axis(table, (jnp.arange(top)[None, :] + turn) % top, axis=1)


def load_shares(count, total, most, skew, full):
    portions = [(1 << 20) // math.isqrt(grade ** skew) + 1 for grade in range(1, count + 1)]
    largest = most if full else min(most, max(-(-total // count), total * portions[0] // sum(portions)))
    least = 1 if total - largest >= count - 1 else 0
    given, rest = [largest] + [least] * (count - 1), total - largest - least * (count - 1)
    while rest > 0:
        candidates = [i for i in range(1, count) if given[i] < largest] or [i for i in range(1, count) if given[i] < most]
        whole, budget = sum([portions[i] for i in candidates]), rest
        for i in candidates:
            extra = min(most - given[i], max(1, budget * portions[i] // whole), rest)
            given[i] = given[i] + extra
            rest = rest - extra
    return np.array(given)


def scatter_about(stream_key, extent, deviation, most, cuts=(), held_as=jnp.bfloat16):
    array = deviation * jax.random.normal(stream_key, extent, jnp.float32)
    if cuts:
        array = array * levels(stream_key, extent, cuts, -0.22, 0.18)
    return jnp.clip(array, -most, most).astype(held_as)


def setup_inputs(seed: int = 0) -> dict:
    key_list = jax.random.split(jax.random.key(seed), 7)
    tokens = scatter_about(key_list[0], (TOKENS, D), 1.0, 6.0, ((0, 16),))
    expert_ids_keys = jax.random.split(jax.random.fold_in(key_list[1], 1), TOKENS // TOK_DEV)
    expert_ids_turns = jax.random.permutation(jax.random.fold_in(key_list[1], 3), TOKENS // TOK_DEV)
    expert_ids = jax.vmap(lambda own, number: shared_out(jax.random.fold_in(key_list[1], 2), own, number, TOK_DEV, EXPERTS, TOPK, CAP, 2))(expert_ids_keys, expert_ids_turns).reshape((TOKENS, TOPK))
    route_weight = jnp.clip(jnp.exp(math.log(0.5) - 2.3025851 * jax.random.uniform(key_list[2], (TOKENS, TOPK), jnp.float32) ** levels(key_list[2], (TOKENS, TOPK), ((0, 16),), -0.2, 0.2)), 0.05, 0.5)
    w_gate = scatter_about(key_list[3], (EXPERTS, D, FF), D ** -0.5, 0.09375, ((0, 16), (2, 2)))
    w_up = scatter_about(key_list[4], (EXPERTS, D, FF), D ** -0.5, 0.09375, ((0, 16), (2, 2)))
    w_down = scatter_about(key_list[5], (EXPERTS, FF, D), FF ** -0.5, 0.1875, ((0, 16), (1, 2)))
    return {"tokens": tokens, "expert_ids": expert_ids, "route_weight": route_weight, "w_gate": w_gate, "w_up": w_up, "w_down": w_down}


def reference(tokens, expert_ids, route_weight, w_gate, w_up, w_down):
    groups = N_ULY * N_DP
    model_width = tokens.shape[1]
    hidden_cut = FF // N_BLK
    grouped = tokens.reshape(groups, TOK_DEV, model_width)
    grouped_ids = expert_ids.reshape(groups, TOK_DEV, TOPK)
    weights = route_weight.reshape(groups, TOK_DEV, TOPK)
    labels = jnp.arange(EXPERTS, dtype=jnp.int32)
    onehot = (grouped_ids[:, :, :, None] == labels[None, None, None, :]).astype(jnp.int32)
    chosen = jnp.sum(onehot, axis=2)
    before = jnp.cumsum(chosen, axis=1) - chosen
    weight_share = jnp.sum(onehot.astype(route_weight.dtype) * weights[:, :, :, None], axis=2)
    positions = jnp.arange(TOK_DEV, dtype=jnp.int32)
    places = jnp.arange(CAP, dtype=jnp.int32)

    def one_expert(running, inputs):
        gate_matrix, up_matrix, down_matrix, picked, slot_rank, scaled = inputs
        matched = ((picked[:, :, None] == 1) & (slot_rank[:, :, None] == places[None, None, :])).astype(jnp.int32)
        source = jnp.sum(matched * positions[None, :, None], axis=1).astype(jnp.int32)
        filled = jnp.sum(matched, axis=1)
        index_full = jnp.broadcast_to(source[:, :, None], (groups, CAP, model_width)).astype(jnp.int32)
        selected = jnp.take_along_axis(grouped, index_full, axis=1)
        selected = jnp.where(filled[:, :, None] == 1, selected, jnp.zeros_like(selected))
        selected = selected.reshape(groups * CAP, model_width)
        gate_sum = jnp.dot(selected, gate_matrix, preferred_element_type=jnp.float32)
        up_sum = jnp.dot(selected, up_matrix, preferred_element_type=jnp.float32)
        hidden = (jax.nn.silu(gate_sum) * up_sum).astype(jnp.bfloat16)
        pieces = jnp.einsum("rbf,bfd->brd",
                            hidden.astype(jnp.float32).reshape(groups * CAP, N_BLK, hidden_cut),
                            down_matrix.astype(jnp.float32).reshape(N_BLK, hidden_cut, model_width))
        pieces = lax.optimization_barrier(pieces.astype(jnp.bfloat16)).astype(jnp.float32)
        answer = jnp.sum(pieces, axis=0).astype(jnp.bfloat16).reshape(groups, CAP, model_width)
        back_index = jnp.broadcast_to(jnp.clip(slot_rank, 0, CAP - 1)[:, :, None], (groups, TOK_DEV, model_width)).astype(jnp.int32)
        gathered = jnp.take_along_axis(answer, back_index, axis=1)
        return running + scaled[:, :, None] * gathered.astype(jnp.float32), None

    start_value = jnp.zeros((groups, TOK_DEV, model_width), jnp.float32)
    inputs = (w_gate, w_up, w_down,
              jnp.transpose(chosen, (2, 0, 1)),
              jnp.transpose(before, (2, 0, 1)),
              jnp.transpose(weight_share, (2, 0, 1)))
    running, _ = lax.scan(one_expert, start_value, inputs)
    return running.reshape(groups * TOK_DEV, model_width).astype(jnp.bfloat16)
```

```python
import jax
import jax.numpy as jnp
from jax import lax
from jax.experimental import pallas as pl
from jax.experimental.pallas import tpu as pltpu
from jax.sharding import PartitionSpec as P


def routing_tables(expert_ids, route_weight, groups, local_count, capacity):
    tokens_here, picks_count = expert_ids.shape
    experts = groups * local_count
    labels = lax.broadcasted_iota(jnp.int32, (1, 1, experts), 2)
    onehot = (expert_ids[:, :, None] == labels).astype(jnp.int32)
    chosen = jnp.sum(onehot, axis=1)
    before = jnp.cumsum(chosen, axis=0) - chosen
    slot_of = jnp.sum(onehot * before[:, None, :], axis=2)
    places = lax.broadcasted_iota(jnp.int32, (1, 1, capacity), 2)
    slot_hot = (slot_of[:, :, None] == places).astype(jnp.float32)
    expert_hot = onehot.astype(jnp.float32).reshape(tokens_here, picks_count, groups, local_count)
    placing = jnp.einsum("tkgl,tkc->gclt", expert_hot, slot_hot)
    placing = placing.reshape(groups * capacity * local_count, tokens_here)
    mixing = jnp.einsum("tkgl,tkc,tk->tgcl", expert_hot, slot_hot, route_weight)
    mixing = mixing.reshape(tokens_here, groups * capacity * local_count)
    return (placing.astype(jnp.bfloat16), mixing)


def local_slots(tokens, expert_ids, route_weight, w_gate, w_up, w_down):
    ulysses_size = lax.axis_size("uly")
    data_size = lax.axis_size("dp")
    cycle_size = lax.axis_size("blk")
    tokens_here, model_width = tokens.shape
    local_count = w_gate.shape[0]
    hidden_cut = w_gate.shape[2]
    groups = ulysses_size * data_size
    experts = groups * local_count
    picks_count = expert_ids.shape[1]
    capacity = min(tokens_here, max(2, 5 * tokens_here * picks_count // (4 * experts)))
    placing, mixing = routing_tables(expert_ids, route_weight, groups, local_count, capacity)
    slice_width = model_width // cycle_size
    rows_total = groups * capacity
    cycle_index = lax.axis_index("blk")
    own_part = lax.dynamic_slice_in_dim(tokens, cycle_index * slice_width, slice_width, 1)
    outgoing = jnp.dot(placing, own_part, preferred_element_type=jnp.float32).astype(jnp.bfloat16)
    outgoing = outgoing.reshape(ulysses_size, data_size, capacity, local_count, slice_width)
    arrived = lax.all_to_all(
        lax.all_to_all(outgoing, "uly", split_axis=0, concat_axis=0, tiled=True),
        "dp",
        split_axis=1,
        concat_axis=1,
        tiled=True,
    )
    arrived = arrived.reshape(rows_total, local_count, slice_width)
    portion = lax.all_gather(arrived, "blk", axis=2, tiled=True)
    gate_more = jnp.einsum("rlw,lwf->rlf", portion, w_gate, preferred_element_type=jnp.float32)
    up_more = jnp.einsum("rlw,lwf->rlf", portion, w_up, preferred_element_type=jnp.float32)
    hidden = (jax.nn.silu(gate_more) * up_more).astype(jnp.bfloat16)
    resplit = lax.all_to_all(w_down, "blk", split_axis=2, concat_axis=1, tiled=True)
    zero_sum = jnp.zeros((slice_width, rows_total * local_count), jnp.float32)
    total = zero_sum
    portion = lax.all_gather(hidden, "blk", axis=2, tiled=True)
    ranges_count = portion.shape[2] // hidden_cut
    for number in range(ranges_count):
        part_hidden = portion[:, :, number * hidden_cut : (number + 1) * hidden_cut]
        part_rows = lax.dynamic_slice_in_dim(resplit, number * hidden_cut, hidden_cut, 1)
        partial_value = jnp.einsum(
            "lfd,rlf->drl", part_rows, part_hidden, preferred_element_type=jnp.float32
        )
        partial_value = partial_value.reshape(slice_width, rows_total * local_count)
        total = total + partial_value.astype(jnp.bfloat16).astype(jnp.float32)
    returned = total.astype(jnp.bfloat16).reshape(
        slice_width, ulysses_size, data_size, capacity, local_count
    )
    returned_rows = lax.all_to_all(
        lax.all_to_all(returned, "uly", split_axis=1, concat_axis=1, tiled=True),
        "dp",
        split_axis=2,
        concat_axis=2,
        tiled=True,
    )
    returned_rows = returned_rows.reshape(slice_width, rows_total * local_count).astype(jnp.float32)
    mixed = lax.dot_general(
        mixing, returned_rows, (((1,), (1,)), ((), ())), precision=lax.Precision.HIGHEST
    )
    return mixed.astype(jnp.bfloat16)


MESH = pl.DeviceIdType.MESH

PLANE, BY_Z, PARTS, SUB = 21 * 128, 0 * 128, 2, 1


def schedule():
    steps = []

    def add(*words):
        for word in words:
            when = word[0] if word[0] in "ei" else ""
            word = word[len(when):]
            steps.append((when, word, word[0], [int(digit) for digit in word[1:]]))

    add("Z10", "iZ20", "X00", "Z11", "iZ21", "X01", "Y100", "eZ20", "iZ30", "X10", "iY200", "Y010")
    add("iZ31", "iX20", "Y101", "eZ21", "iY201", "X11", "Y011", "C0", "G00", "eZ30", "eX20", "eY200")
    add("iX21", "iY300", "G01", "Y110", "D00", "D01", "eY201", "eZ31", "eX21", "iX30", "iY301", "iY210")
    add("iX31", "Y111", "iM00", "iM01", "iY211", "C1", "G10", "eX30", "eY300", "G11", "eY210", "iY310")
    add("D10", "D11", "eX31", "eY301", "eM00", "eM01", "eY211", "iY311", "C2", "G20", "eY310", "iF020")
    add("G21", "eY311", "iF000", "ia0", "D20", "iF030", "D21", "eF020", "C3", "G30", "eF000", "iF010")
    add("M20", "G31", "eF030", "M21", "D30", "eF010", "D31", "ib00", "ib10", "M30", "M31", "F200")
    add("F220", "eA20", "iM10", "iM11", "F210", "F230", "eM10", "eM11", "F300", "iF320", "iF310", "iF330")
    add("S300", "eF320", "eS320", "eF310", "eS310", "eF330", "eS330", "eB200", "eS210", "eB210", "eS230", "F100")
    add("F120", "A10", "iS320", "F110", "F130", "iS310", "iS200", "iS330", "B100", "iB110", "iS220", "S110")
    add("eB110", "iS210", "S130", "eL00", "eL20", "ea0", "iS230", "L10", "L30", "eb00", "eb10")
    return steps


SCHEDULE = schedule()


def neighbours(deep):
    at_y, at_u, at_z = lax.axis_index("blk"), lax.axis_index("uly"), lax.axis_index("dp")
    at_x, core = at_u // 2, at_u % 2
    devices = {
        "up": {"dp": jnp.minimum(at_z + 1, deep - 1)},
        "down": {"dp": jnp.maximum(at_z - 1, 0)},
        "x": {"uly": (1 - at_x) * 2 + core},
        "y": {"blk": 1 - at_y},
        "core": {"uly": at_x * 2 + 1 - core},
    }
    return at_x, at_y, at_z, core, devices


def greet_all(deep, at_z, devices):
    barrier = pltpu.get_barrier_semaphore()
    for name in ("x", "y", "core"):
        pl.semaphore_signal(barrier, inc=1, device_id=devices[name], device_id_type=MESH)

    @pl.when(at_z > 0)
    def _():
        pl.semaphore_signal(barrier, inc=1, device_id=devices["down"], device_id_type=MESH)

    @pl.when(at_z < deep - 1)
    def _():
        pl.semaphore_signal(barrier, inc=1, device_id=devices["up"], device_id_type=MESH)


def greet_wait(deep, at_z):
    barrier = pltpu.get_barrier_semaphore()
    beside = (at_z > 0).astype(jnp.int32) + (at_z < deep - 1).astype(jnp.int32)
    pl.semaphore_wait(barrier, 3 + beside)


def orders(deep):
    return [sorted(range(deep), key=lambda p: (abs(p - z), (p < z) == (2 * z < deep))) for z in range(deep)]


def fused_kernel(deep, plane, by_z, parts, tok, ids_hbm, weight_hbm, gate_hbm, up_hbm, down_hbm, out,
                 every, w_gate, w_up, w_down, ids, weight, hidden, part, total, ya, xb, zin, fin, own_sem, send, recv):
    at_x, at_y, at_z, core, devices = neighbours(deep)
    rows_each, width = tok.shape
    wide = every.shape[1]
    half_width = width // 2
    piece = rows_each // parts
    slab = rows_each // 2
    slice_rows = slab // SUB
    apart = wide - plane
    low, high = at_z > 0, at_z < deep - 1
    ends = (at_z == 0) | (at_z == deep - 1)
    inner = (at_z > 0) & (at_z < deep - 1)
    first_cols = at_y * apart
    plane_cols = pl.ds(pl.multiple_of(first_cols, 128), plane)
    theirs = pl.ds(pl.multiple_of(at_y * plane, 128), apart)
    lacking = pl.ds(pl.multiple_of((1 - at_y) * plane, 128), apart)
    x_cols = pl.ds(pl.multiple_of(first_cols + at_y * by_z, 128), plane - by_z)
    z_cols = pl.ds(pl.multiple_of(first_cols + (1 - at_y) * (plane - by_z), 128), max(by_z, 128))
    entire = pl.ds(0, wide)
    arrivals = orders(deep)

    def table(rows, k):
        return sum((at_z == z).astype(jnp.int32) * rows[z][k] for z in range(deep))

    planes = [at_z] + [table(arrivals, k) for k in range(1, deep)]
    pending = []
    only = [None]

    def device(to):
        return devices[to] if isinstance(to, str) else to

    def copy(src, dst, kind, index, to):
        return pltpu.make_async_remote_copy(
            src_ref=src, dst_ref=dst, send_sem=send.at[kind, index], recv_sem=recv.at[kind, index],
            device_id=device(to), device_id_type=MESH)

    def start(condition, *what):
        def go():
            copy(*what).start()

        if only[0] is not None:
            condition = only[0] if condition is None else only[0] & condition
        if condition is None:
            go()
        else:
            pl.when(condition)(go)
        pending.append((condition, what))

    def do(go):
        if only[0] is None:
            go()
        else:
            pl.when(only[0])(go)

    def given(condition, act):
        before = only[0]
        only[0] = condition if before is None else before & condition
        act()
        only[0] = before

    def arrive(dst, kind, index):
        do(lambda: copy(dst, dst, kind, index, "x").wait_recv())

    def block(x_of, core_of, z_of, p, cols):
        first = (z_of * 4 + 2 * x_of + core_of) * rows_each + p * piece
        return every.at[pl.ds(pl.multiple_of(first, piece), piece), cols]

    def from_below(z_of):
        return z_of < at_z

    def toward(step):
        return {"dp": jnp.clip(at_z + step, 0, deep - 1)}

    def within(z_of):
        return (z_of >= 0) & (z_of < deep)

    def z_arrives(k, p):
        z_of = planes[k]
        index = z_of * parts + p
        step = jnp.where(from_below(z_of), 1, -1)
        kind = jnp.where(from_below(z_of), 0, 1)
        held = block(at_x, core, z_of, p, plane_cols)
        arrive(held, kind, index)
        start(within(at_z + step), held, held, kind, index, toward(step))
        along = block(at_x, core, z_of, p, x_cols)
        start(None, along, along, 4, index, "x")
        sent = block(at_x, core, z_of, p, theirs)
        start(None, sent, sent, 5, index, "y")
        start(None, held, held, 7, index, "core")

    def x_arrives(k, p):
        z_of = planes[k]
        index = z_of * parts + p
        held = block(1 - at_x, core, z_of, p, plane_cols if k == 0 else x_cols)
        arrive(held, 4, index)
        sent = block(1 - at_x, core, z_of, p, theirs)
        start(None, sent, sent, 6, index, "y")
        if k == 0 and by_z:
            extra = block(1 - at_x, core, z_of, p, z_cols)
            start(high, extra, extra, 2, index, "up")
            start(low, extra, extra, 3, index, "down")
        start(None, held, held, 9, index, "core")

    def h_arrives(k, p):
        z_of = planes[k]
        index = z_of * parts + p
        step = jnp.where(from_below(z_of), 1, -1)
        kind = jnp.where(from_below(z_of), 2, 3)
        held = block(1 - at_x, core, z_of, p, z_cols)
        arrive(held, kind, index)
        start(within(at_z + step), held, held, kind, index, toward(step))
        start(None, held, held, 10, index, "core")

    def y_arrives(k, other, p):
        z_of = planes[k]
        index = z_of * parts + p
        held = block(1 - at_x if other else at_x, core, z_of, p, lacking)
        arrive(held, 6 if other else 5, index)
        start(None, held, held, 11 if other else 8, index, "core")

    def complete(k):
        z_of = planes[k]
        for p in range(parts):
            index = z_of * parts + p
            arrive(block(at_x, 1 - core, z_of, p, entire if k == 0 else plane_cols), 7, index)
            if k > 0:
                arrive(block(at_x, 1 - core, z_of, p, lacking), 8, index)
                if by_z:
                    arrive(block(1 - at_x, 1 - core, z_of, p, z_cols), 10, index)
            arrive(block(1 - at_x, 1 - core, z_of, p, plane_cols if k == 0 else x_cols), 9, index)
            arrive(block(1 - at_x, 1 - core, z_of, p, lacking), 11, index)

    batch = 4 * rows_each
    expert = (2 * at_x + core) * deep + at_z
    experts = 4 * deep

    def gate_up(k, n):
        span = w_gate.shape[1] // 2
        rows = pl.ds(pl.multiple_of(planes[k] * batch, batch), batch)
        cols = pl.ds(n * span, span)
        features = every[rows, 0:width]
        gate = jnp.dot(features, w_gate[:, cols], preferred_element_type=jnp.float32)
        up = jnp.dot(features, w_up[:, cols], preferred_element_type=jnp.float32)
        shares = every[rows, width:wide].astype(jnp.float32)
        lane = lax.broadcasted_iota(jnp.int32, shares.shape, 1)
        mine = (lane == expert) | (lane == expert + experts)
        share = jnp.sum(jnp.where(mine, shares, 0.0), axis=1, keepdims=True)
        hidden[:, cols] = (jax.nn.silu(gate) * up * share).astype(jnp.bfloat16)

    def down(k, n):
        half = (1 - at_y) if n == 0 else at_y
        span = half_width // 2
        z_of = planes[k]

        @pl.loop(0, 2)
        def _(m):
            cols = pl.ds(pl.multiple_of(half * half_width + m * span, span), span)
            value = jnp.dot(hidden[...], w_down[:, cols], preferred_element_type=jnp.float32).astype(jnp.bfloat16)
            into = pl.ds(pl.multiple_of(m * span, span), span)
            for g in range(4):
                part[z_of, g, half, :, into] = value[g * rows_each:(g + 1) * rows_each]

        for x_of in range(2):
            start(None, part.at[z_of, 2 * x_of + 1 - core, half], total.at[z_of, x_of, half],
                  12, (z_of * 2 + x_of) * 2 + half, "core")

    upper, lower = pl.ds(0, slab), pl.ds(slab, slab)

    def added(one, other):
        return (one.astype(jnp.float32) + other.astype(jnp.float32)).astype(jnp.bfloat16)

    def strip(base, s):
        return pl.ds(base + s * slice_rows, slice_rows)

    def halves_meet(k, n):
        half = (1 - at_y) if n == 0 else at_y
        z_of = planes[k]
        for x_of in (1 - at_x, at_x):
            spot = total.at[z_of, x_of, half]
            arrive(spot, 12, (z_of * 2 + x_of) * 2 + half)
            add_to(spot, part.at[z_of, 2 * x_of + core, half])
            for s in range(SUB):
                if n == 0:
                    start(None, total.at[z_of, x_of, half, strip(0, s)], ya.at[z_of, x_of, strip(0, s)],
                          13, (z_of * 2 + x_of) * SUB + s, "y")
                if x_of is not at_x:
                    start(None, total.at[z_of, x_of, half, strip(slab, s)], xb.at[z_of, half, strip(0, s)],
                          14, (z_of * 2 + half) * SUB + s, "x")

    def quarter(z_of, q, s):
        if q < 2:
            return total.at[z_of, (1 - at_x) if q == 0 else at_x, at_y, strip(0, s)]
        return total.at[z_of, at_x, (1 - at_y) if q == 2 else at_y, strip(slab, s)]

    def add_to(spot, other):
        def go():
            spot[...] = added(spot[...], other[...])

        do(go)

    def first_sum(k, q, s):
        z_of = planes[k]
        if q < 2:
            x_of = (1 - at_x) if q == 0 else at_x
            came, kind, index = ya.at[z_of, x_of, strip(0, s)], 13, z_of * 2 + x_of
        else:
            half = (1 - at_y) if q == 2 else at_y
            came, kind, index = xb.at[z_of, half, strip(0, s)], 14, z_of * 2 + half
        arrive(came, kind, index * SUB + s)
        add_to(quarter(z_of, q, s), came)

    def second_send(k, s):
        z_of = planes[k]
        for n, to in ((0, "x"), (1, "y")):
            start(None, quarter(z_of, 2 * n, s), fin.at[z_of, n, strip(0, s)], 17 + n, z_of * SUB + s, to)

    def second_sum(k, n, s):
        z_of = planes[k]
        came = fin.at[z_of, n, strip(0, s)]
        arrive(came, 17 + n, z_of * SUB + s)
        add_to(quarter(z_of, 2 * n + 1, s), came)

    def z_stage(k, q, s):
        z_of = planes[k]
        rises = z_of > at_z
        step = jnp.where(rises, 1, -1)
        side = jnp.where(rises, 0, 1)
        index = (z_of * 4 + q) * SUB + s
        spot = quarter(z_of, q, s)
        came = zin.at[side, z_of, q, strip(0, s)]

        def inbound():
            arrive(came, 15 + side, index)
            add_to(spot, came)

        given(within(at_z - step), inbound)
        start(None, spot, came, 15 + side, index, toward(step))

    def z_last(q, s):
        for side, condition in ((0, low), (1, high)):
            def inbound(side=side):
                came = zin.at[side, at_z, q, strip(0, s)]
                arrive(came, 15 + side, (at_z * 4 + q) * SUB + s)
                add_to(quarter(at_z, q, s), came)

            given(condition, inbound)

    mine = pl.ds(pl.multiple_of((at_z * 4 + 2 * at_x + core) * rows_each, rows_each), rows_each)
    placed = pltpu.make_async_copy(tok, every.at[mine, pl.ds(0, width)], own_sem.at[0])
    placed.start()
    weights = [pltpu.make_async_copy(src, dst, own_sem.at[1 + n])
               for n, (src, dst) in enumerate(((gate_hbm, w_gate), (up_hbm, w_up), (down_hbm, w_down)))]
    for each in weights:
        each.start()
    picks = [pltpu.make_async_copy(src, dst, own_sem.at[4 + n])
             for n, (src, dst) in enumerate(((ids_hbm, ids), (weight_hbm, weight)))]
    for each in picks:
        each.start()
    greet_all(deep, at_z, devices)
    for each in picks:
        each.wait()
    shape = (wide - width, rows_each)
    lane = lax.broadcasted_iota(jnp.int32, shape, 0)
    named = jnp.where(lane < experts, lane, lane - experts)
    scaled = jnp.zeros(shape, jnp.float32)
    for pick in range(ids.shape[0]):
        scaled = scaled + jnp.where(ids[pick:pick + 1, :] == named, weight[pick:pick + 1, :], 0.0)
    rough = scaled.astype(jnp.bfloat16).astype(jnp.float32)
    every[mine, width:wide] = jnp.where(lane < experts, rough, scaled - rough).T.astype(jnp.bfloat16)
    with jax.named_scope("greet"):
        greet_wait(deep, at_z)
    with jax.named_scope("placed"):
        placed.wait()
    for p in range(parts):
        index = at_z * parts + p
        held = block(at_x, core, at_z, p, plane_cols)
        start(high, held, held, 0, index, "up")
        start(low, held, held, 1, index, "down")
        start(None, held, held, 4, index, "x")
    for p in range(parts):
        whole = block(at_x, core, at_z, p, entire)
        start(None, whole, whole, 7, at_z * parts + p, "core")

    acts = {
        "Z": z_arrives, "X": x_arrives, "H": h_arrives, "Y": y_arrives, "C": complete,
        "G": gate_up, "D": down, "M": halves_meet,
        "F": first_sum, "A": second_send, "B": second_sum, "S": z_stage, "L": z_last,
        "a": lambda s: second_send(0, s),
        "b": lambda n, s: second_sum(0, n, s),
    }
    waited = [False]
    for when, word, name, numbers in SCHEDULE:
        if name == "G" and not waited[0]:
            waited[0] = True
            with jax.named_scope("weights"):
                for each in weights:
                    each.wait()
        only[0] = {"": None, "e": ends, "i": inner}[when]
        with jax.named_scope(word):
            acts[name](*numbers)
    only[0] = None
    out[...] = total[at_z, at_x, at_y]
    with jax.named_scope("drain"):
        for condition, what in pending:
            def end(what=what):
                copy(*what).wait_send()

            if condition is None:
                end()
            else:
                pl.when(condition)(end)


def local_dense(tokens, expert_ids, route_weight, w_gate, w_up, w_down):
    deep = lax.axis_size("dp")
    rows_each, width = tokens.shape
    hidden_cut = w_gate.shape[2]
    half = width // 2
    wide = width + 128
    plane = PLANE
    by_z = BY_Z
    parts = PARTS
    slab = rows_each // 2
    kind = tokens.dtype
    vmem = pl.BlockSpec(memory_space=pltpu.VMEM)
    hbm = pl.BlockSpec(memory_space=pl.ANY)
    return pl.pallas_call(
        lambda *refs: fused_kernel(deep, plane, by_z, parts, *refs),
        out_shape=jax.ShapeDtypeStruct((rows_each, half), kind),
        in_specs=[hbm] * 6,
        out_specs=vmem,
        scratch_shapes=[
            pltpu.VMEM((deep * 4 * rows_each, wide), kind),
            pltpu.VMEM((width, hidden_cut), kind),
            pltpu.VMEM((width, hidden_cut), kind),
            pltpu.VMEM((hidden_cut, width), kind),
            pltpu.VMEM(expert_ids.shape[::-1], expert_ids.dtype),
            pltpu.VMEM(route_weight.shape[::-1], route_weight.dtype),
            pltpu.VMEM((4 * rows_each, hidden_cut), kind),
            pltpu.VMEM((deep, 4, 2, rows_each, half), kind),
            pltpu.VMEM((deep, 2, 2, rows_each, half), kind),
            pltpu.VMEM((deep, 2, slab, half), kind),
            pltpu.VMEM((deep, 2, slab, half), kind),
            pltpu.VMEM((2, deep, 4, slab, half), kind),
            pltpu.VMEM((deep, 2, slab, half), kind),
            pltpu.SemaphoreType.DMA((6,)),
            pltpu.SemaphoreType.DMA((19, deep * 4 * max(SUB, PARTS // 2))),
            pltpu.SemaphoreType.DMA((19, deep * 4 * max(SUB, PARTS // 2))),
        ],
        compiler_params=pltpu.CompilerParams(
            collective_id=0, has_side_effects=True, vmem_limit_bytes=60 << 20),
    )(tokens, expert_ids.T, route_weight.T, w_gate[0], w_up[0], w_down[0])


def solution(mesh):
    dense = mesh.shape["blk"] == 2 and mesh.shape["uly"] == 4 and mesh.shape["dp"] == 4
    return jax.shard_map(
        local_dense if dense else local_slots,
        mesh=mesh,
        in_specs=(
            P(("uly", "dp"), None),
            P(("uly", "dp"), None),
            P(("uly", "dp"), None),
            P(("uly", "dp"), None, "blk"),
            P(("uly", "dp"), None, "blk"),
            P(("uly", "dp"), "blk", None),
        ),
        out_specs=P(("uly", "dp"), "blk"),
        check_vma=False,
    )
```

```python
import jax
import jax.numpy as jnp
from jax import lax
from jax.experimental import pallas as pl
from jax.experimental.pallas import tpu as pltpu
from jax.sharding import PartitionSpec as P


def routing_tables(expert_ids, route_weight, groups, local_count, capacity):
    tokens_here, picks_count = expert_ids.shape
    experts = groups * local_count
    labels = lax.broadcasted_iota(jnp.int32, (1, 1, experts), 2)
    onehot = (expert_ids[:, :, None] == labels).astype(jnp.int32)
    chosen = jnp.sum(onehot, axis=1)
    before = jnp.cumsum(chosen, axis=0) - chosen
    slot_of = jnp.sum(onehot * before[:, None, :], axis=2)
    places = lax.broadcasted_iota(jnp.int32, (1, 1, capacity), 2)
    slot_hot = (slot_of[:, :, None] == places).astype(jnp.float32)
    expert_hot = onehot.astype(jnp.float32).reshape(tokens_here, picks_count, groups, local_count)
    placing = jnp.einsum("tkgl,tkc->gclt", expert_hot, slot_hot)
    placing = placing.reshape(groups * capacity * local_count, tokens_here)
    mixing = jnp.einsum("tkgl,tkc,tk->tgcl", expert_hot, slot_hot, route_weight)
    mixing = mixing.reshape(tokens_here, groups * capacity * local_count)
    return (placing.astype(jnp.bfloat16), mixing)


def local_slots(tokens, expert_ids, route_weight, w_gate, w_up, w_down):
    ulysses_size = lax.axis_size("uly")
    data_size = lax.axis_size("dp")
    cycle_size = lax.axis_size("blk")
    tokens_here, model_width = tokens.shape
    local_count = w_gate.shape[0]
    hidden_cut = w_gate.shape[2]
    groups = ulysses_size * data_size
    experts = groups * local_count
    picks_count = expert_ids.shape[1]
    capacity = min(tokens_here, max(2, 5 * tokens_here * picks_count // (4 * experts)))
    placing, mixing = routing_tables(expert_ids, route_weight, groups, local_count, capacity)
    slice_width = model_width // cycle_size
    rows_total = groups * capacity
    cycle_index = lax.axis_index("blk")
    own_part = lax.dynamic_slice_in_dim(tokens, cycle_index * slice_width, slice_width, 1)
    outgoing = jnp.dot(placing, own_part, preferred_element_type=jnp.float32).astype(jnp.bfloat16)
    outgoing = outgoing.reshape(ulysses_size, data_size, capacity, local_count, slice_width)
    arrived = lax.all_to_all(
        lax.all_to_all(outgoing, "uly", split_axis=0, concat_axis=0, tiled=True),
        "dp",
        split_axis=1,
        concat_axis=1,
        tiled=True,
    )
    arrived = arrived.reshape(rows_total, local_count, slice_width)
    portion = lax.all_gather(arrived, "blk", axis=2, tiled=True)
    gate_more = jnp.einsum("rlw,lwf->rlf", portion, w_gate, preferred_element_type=jnp.float32)
    up_more = jnp.einsum("rlw,lwf->rlf", portion, w_up, preferred_element_type=jnp.float32)
    hidden = (jax.nn.silu(gate_more) * up_more).astype(jnp.bfloat16)
    resplit = lax.all_to_all(w_down, "blk", split_axis=2, concat_axis=1, tiled=True)
    zero_sum = jnp.zeros((slice_width, rows_total * local_count), jnp.float32)
    total = zero_sum
    portion = lax.all_gather(hidden, "blk", axis=2, tiled=True)
    ranges_count = portion.shape[2] // hidden_cut
    for number in range(ranges_count):
        part_hidden = portion[:, :, number * hidden_cut : (number + 1) * hidden_cut]
        part_rows = lax.dynamic_slice_in_dim(resplit, number * hidden_cut, hidden_cut, 1)
        partial_value = jnp.einsum(
            "lfd,rlf->drl", part_rows, part_hidden, preferred_element_type=jnp.float32
        )
        partial_value = partial_value.reshape(slice_width, rows_total * local_count)
        total = total + partial_value.astype(jnp.bfloat16).astype(jnp.float32)
    returned = total.astype(jnp.bfloat16).reshape(
        slice_width, ulysses_size, data_size, capacity, local_count
    )
    returned_rows = lax.all_to_all(
        lax.all_to_all(returned, "uly", split_axis=1, concat_axis=1, tiled=True),
        "dp",
        split_axis=2,
        concat_axis=2,
        tiled=True,
    )
    returned_rows = returned_rows.reshape(slice_width, rows_total * local_count).astype(jnp.float32)
    mixed = lax.dot_general(
        mixing, returned_rows, (((1,), (1,)), ((), ())), precision=lax.Precision.HIGHEST
    )
    return mixed.astype(jnp.bfloat16)


MESH = pl.DeviceIdType.MESH

PLANE, BY_Z, PARTS, SUB = 22 * 128, 2 * 128, 4, 2
VMEM_LIMIT = 67043328 - (288 << 10)


SCHEDULE = (
    100, 200200, 1000, 110, 200210, 1010, 120, 200220, 1020, 3100, 203200, 200130,
    200230, 202200, 202210, 201030, 3010, 100130, 101030, 3101, 202220, 201100, 200300, 203201,
    202100, 3011, 101100, 100200, 202230, 201200, 3102, 102100, 200310, 202110, 203202, 201110,
    3012, 101110, 200320, 202120, 3103, 100210, 102110, 201210, 203203, 200330, 202300, 202310,
    202130, 202320, 201120, 202330, 3013, 101120, 3110, 100220, 102120, 201220, 203300, 4000,
    5000, 203210, 1130, 103200, 103111, 100230, 5010, 102130, 101200, 103201, 103112, 203301,
    203111, 6000, 100300, 102200, 101210, 103202, 201230, 203302, 6010, 103113, 101220, 100310,
    102210, 103203, 103210, 101230, 100320, 102220, 103300, 1300, 3211, 100330, 102300, 203303,
    201310, 203112, 3212, 102310, 102230, 102320, 102330, 101310, 103301, 201320, 203113, 3213,
    101320, 103302, 201330, 3310, 101330, 103303, 3311, 3312, 3313, 4300, 5300, 7000,
    7010, 5310, 6300, 6310, 4200, 5200, 8000, 8020, 213000, 7300, 5210, 8001,
    8021, 213100, 7310, 6200, 8010, 8030, 6210, 8011, 8031, 4100, 5100, 108300,
    110300, 108320, 110320, 214000, 214100, 7200, 5110, 108301, 110301, 108321, 110321, 208300,
    208320, 7210, 108310, 110310, 108330, 110330, 6100, 208301, 208321, 6110, 208310, 214010,
    210300, 8311, 110311, 208330, 207100, 210320, 207110, 8331, 110331, 214110, 210301, 8200,
    8220, 109200, 107100, 210321, 210200, 8201, 8221, 109210, 107110, 210310, 210220, 8210,
    8230, 210330, 210201, 8211, 8231, 111200, 110210, 111210, 110230, 210311, 210221, 8100,
    8120, 9100, 112000, 210331, 210210, 8101, 8121, 9110, 112200, 113000, 111201, 210230,
    208110, 208130, 10211, 108110, 112010, 8111, 108130, 112210, 113100, 111211, 208131, 10231,
    108131, 112100, 11100, 10110, 11110, 10130, 112300, 11101, 10111, 11111, 10131, 212100,
    212300, 12110, 114000, 114100, 12310, 114010, 114110,
)


def neighbours(deep):
    at_y, at_u, at_z = lax.axis_index("blk"), lax.axis_index("uly"), lax.axis_index("dp")
    at_x, core = at_u // 2, at_u % 2
    devices = {
        "up": {"dp": jnp.minimum(at_z + 1, deep - 1)},
        "down": {"dp": jnp.maximum(at_z - 1, 0)},
        "x": {"uly": (1 - at_x) * 2 + core},
        "y": {"blk": 1 - at_y},
        "core": {"uly": at_x * 2 + 1 - core},
    }
    return at_x, at_y, at_z, core, devices


def greet_all(deep, at_z, devices):
    barrier = pltpu.get_barrier_semaphore()
    for name in ("x", "y", "core"):
        pl.semaphore_signal(barrier, inc=1, device_id=devices[name], device_id_type=MESH)

    @pl.when(at_z > 0)
    def _():
        pl.semaphore_signal(barrier, inc=1, device_id=devices["down"], device_id_type=MESH)

    @pl.when(at_z < deep - 1)
    def _():
        pl.semaphore_signal(barrier, inc=1, device_id=devices["up"], device_id_type=MESH)


def greet_wait(deep, at_z):
    barrier = pltpu.get_barrier_semaphore()
    beside = (at_z > 0).astype(jnp.int32) + (at_z < deep - 1).astype(jnp.int32)
    pl.semaphore_wait(barrier, 3 + beside)


def semaphore_slots(deep):
    pieces, extra = deep * PARTS, deep * PARTS if BY_Z else 0
    return (
        ("z", pieces), ("h", extra), ("x", pieces), ("ys", pieces), ("yo", pieces), ("c", deep), ("m", deep * 2),
        ("fy", deep * 2 * SUB), ("fx", deep * 2 * SUB), ("s", deep * 4 * SUB), ("t", 4 * SUB),
        ("bx", deep * SUB), ("by", deep * SUB),
    )


def orders(deep):
    return [sorted(range(deep), key=lambda p: (abs(p - z), (p < z) == (2 * z < deep))) for z in range(deep)]


def fused_kernel(deep, plane, by_z, parts, tok, ids_hbm, weight_hbm, gate_hbm, up_hbm, down_hbm, out,
                 every, w_gate, w_up, w_down, ids, weight, hidden, part, total, ya, xb, zin, fin, own_sem, send, recv):
    at_x, at_y, at_z, core, devices = neighbours(deep)
    rows_each, width = tok.shape
    wide = every.shape[1]
    half_width = width // 2
    piece = rows_each // parts
    slab = rows_each // 2
    slice_rows = slab // SUB
    apart = wide - plane
    low, high = at_z > 0, at_z < deep - 1
    ends = (at_z == 0) | (at_z == deep - 1)
    inner = (at_z > 0) & (at_z < deep - 1)
    first_cols = at_y * apart
    plane_cols = pl.ds(pl.multiple_of(first_cols, 128), plane)
    theirs = pl.ds(pl.multiple_of(at_y * plane, 128), apart)
    lacking = pl.ds(pl.multiple_of((1 - at_y) * plane, 128), apart)
    x_cols = pl.ds(pl.multiple_of(first_cols + at_y * by_z, 128), plane - by_z)
    z_cols = pl.ds(pl.multiple_of(first_cols + (1 - at_y) * (plane - by_z), 128), max(by_z, 128))
    entire = pl.ds(0, wide)
    arrivals = orders(deep)

    def table(rows, k):
        return sum((at_z == z).astype(jnp.int32) * rows[z][k] for z in range(deep))

    planes = [at_z] + [table(arrivals, k) for k in range(1, deep)]
    pending = []
    only = [None]

    def device(to):
        return devices[to] if isinstance(to, str) else to

    slots, count = {}, 0
    for name, size in semaphore_slots(deep):
        slots[name] = count
        count += size
    names = ("z", "h", "x", "x0", "ys", "yo", "cz", "cz0", "cx", "cx0", "ch", "cys", "cyo", "m", "fy", "fx", "s", "s0", "bx", "by")
    sends = {name: number for number, name in enumerate(names)}

    def copy(src, dst, send_at, recv_at, to):
        return pltpu.make_async_remote_copy(
            src_ref=src, dst_ref=dst, send_sem=send.at[send_at], recv_sem=recv.at[recv_at],
            device_id=device(to), device_id_type=MESH)

    def start(condition, src, dst, kind, index, to, other=None):
        what = (src, dst, other if other is not None and not isinstance(other, str) else sends[other or kind], slots[kind] + index, to)

        def go():
            copy(*what).start()

        if only[0] is not None:
            condition = only[0] if condition is None else only[0] & condition
        if condition is None:
            go()
        else:
            pl.when(condition)(go)
        pending.append((condition, what))

    def do(go):
        if only[0] is None:
            go()
        else:
            pl.when(only[0])(go)

    def given(condition, act):
        before = only[0]
        only[0] = condition if before is None else before & condition
        act()
        only[0] = before

    def arrive(dst, kind, index):
        at = slots[kind] + index
        do(lambda: copy(dst, dst, at, at, "x").wait_recv())

    def group_rows(x_of, core_of, z_of, cols):
        first = (z_of * 4 + 2 * x_of + core_of) * rows_each
        return every.at[pl.ds(pl.multiple_of(first, rows_each), rows_each), cols]

    seen, doubled, stages = {}, set(), {}

    def pass_on(key, held, kind, z_of):
        done = {}
        for kind_of in (1, 2):
            if word_for[0] in (0, kind_of):
                seen[key, kind_of] = seen.get((key, kind_of), 0) + 1
                done[kind_of] = seen[key, kind_of] == parts
        whole = [name for name in done if done[name]]
        if not whole:
            return
        if len(whole) == len(done):
            start(None, held, held, "c", z_of, "core", kind)
        else:
            given(ends if whole[0] == 1 else inner, lambda: start(None, held, held, "c", z_of, "core", kind))

    word_for = [0]

    def block(x_of, core_of, z_of, p, cols):
        first = (z_of * 4 + 2 * x_of + core_of) * rows_each + p * piece
        return every.at[pl.ds(pl.multiple_of(first, piece), piece), cols]

    def from_below(z_of):
        return z_of < at_z

    def toward(step):
        return {"dp": jnp.clip(at_z + step, 0, deep - 1)}

    def within(z_of):
        return (z_of >= 0) & (z_of < deep)

    def z_arrives(k, p):
        z_of = planes[k]
        index = z_of * parts + p
        step = jnp.where(from_below(z_of), 1, -1)
        held = block(at_x, core, z_of, p, plane_cols)
        arrive(held, "z", index)
        start(within(at_z + step), held, held, "z", index, toward(step))
        along = block(at_x, core, z_of, p, x_cols)
        start(None, along, along, "x", index, "x")
        sent = block(at_x, core, z_of, p, theirs)
        start(None, sent, sent, "ys", index, "y")
        pass_on(("z", k), group_rows(at_x, core, z_of, plane_cols), "cz", z_of)

    def x_arrives(k, p):
        z_of = planes[k]
        index = z_of * parts + p
        cols = plane_cols if k == 0 else x_cols
        held = block(1 - at_x, core, z_of, p, cols)
        arrive(held, "x", index)
        sent = block(1 - at_x, core, z_of, p, theirs)
        start(None, sent, sent, "yo", index, "y")
        if k == 0 and by_z:
            extra = block(1 - at_x, core, z_of, p, z_cols)
            start(high, extra, extra, "h", index, "up")
            start(low, extra, extra, "h", index, "down")
        pass_on(("x", k), group_rows(1 - at_x, core, z_of, cols), "cx" if k else "cx0", z_of)

    def h_arrives(k, p):
        z_of = planes[k]
        index = z_of * parts + p
        step = jnp.where(from_below(z_of), 1, -1)
        held = block(1 - at_x, core, z_of, p, z_cols)
        arrive(held, "h", index)
        start(within(at_z + step), held, held, "h", index, toward(step))
        pass_on(("h", k), group_rows(1 - at_x, core, z_of, z_cols), "ch", z_of)

    def y_arrives(k, other, p):
        z_of = planes[k]
        index = z_of * parts + p
        x_of = 1 - at_x if other else at_x
        arrive(block(x_of, core, z_of, p, lacking), "yo" if other else "ys", index)
        pass_on(("y", k, other), group_rows(x_of, core, z_of, lacking), "cyo" if other else "cys", z_of)

    def complete(k):
        arrive(every.at[pl.ds(0, 2 * rows_each), :], "c", planes[k])

    batch = 4 * rows_each
    expert = (2 * at_x + core) * deep + at_z
    experts = 4 * deep

    def gate_up(k, n):
        span = w_gate.shape[1] // 2
        rows = pl.ds(pl.multiple_of(planes[k] * batch, batch), batch)
        cols = pl.ds(n * span, span)
        features = every[rows, 0:width]
        gate = jnp.dot(features, w_gate[:, cols], preferred_element_type=jnp.float32)
        up = jnp.dot(features, w_up[:, cols], preferred_element_type=jnp.float32)
        shares = every[rows, width:wide].astype(jnp.float32)
        lane = lax.broadcasted_iota(jnp.int32, shares.shape, 1)
        mine = (lane == expert) | (lane == expert + experts)
        share = jnp.sum(jnp.where(mine, shares, 0.0), axis=1, keepdims=True)
        hidden[:, cols] = (jax.nn.silu(gate) * up * share).astype(jnp.bfloat16)

    def down(k, n):
        half = (1 - at_y) if n == 0 else at_y
        span = half_width // 2
        z_of = planes[k]

        @pl.loop(0, 2)
        def _(m):
            cols = pl.ds(pl.multiple_of(half * half_width + m * span, span), span)
            value = jnp.dot(hidden[...], w_down[:, cols], preferred_element_type=jnp.float32).astype(jnp.bfloat16)
            into = pl.ds(pl.multiple_of(m * span, span), span)
            for g in range(4):
                part[z_of, g, half, :, into] = value[g * rows_each:(g + 1) * rows_each]

        for x_of in range(2):
            start(None, part.at[z_of, 2 * x_of + 1 - core, half], total.at[z_of, x_of, half],
                  "m", z_of * 2 + half, "core")

    upper, lower = pl.ds(0, slab), pl.ds(slab, slab)

    def added(one, other):
        return (one.astype(jnp.float32) + other.astype(jnp.float32)).astype(jnp.bfloat16)

    def strip(base, s):
        return pl.ds(base + s * slice_rows, slice_rows)

    def halves_meet(k, n):
        half = (1 - at_y) if n == 0 else at_y
        z_of = planes[k]
        arrive(total.at[z_of, :, half], "m", z_of * 2 + half)
        for x_of in (1 - at_x, at_x):
            spot = total.at[z_of, x_of, half]
            add_to(spot, part.at[z_of, 2 * x_of + core, half])
            for s in range(SUB):
                if n == 0:
                    start(None, total.at[z_of, x_of, half, strip(0, s)], ya.at[z_of, x_of, strip(0, s)],
                          "fy", (z_of * 2 + x_of) * SUB + s, "y")
                if x_of is not at_x:
                    start(None, total.at[z_of, x_of, half, strip(slab, s)], xb.at[z_of, half, strip(0, s)],
                          "fx", (z_of * 2 + half) * SUB + s, "x")

    def quarter(z_of, q, s):
        if q < 2:
            return total.at[z_of, (1 - at_x) if q == 0 else at_x, at_y, strip(0, s)]
        return total.at[z_of, at_x, (1 - at_y) if q == 2 else at_y, strip(slab, s)]

    def add_to(spot, other):
        def go():
            spot[...] = added(spot[...], other[...])

        do(go)

    def first_sum(k, q, s):
        z_of = planes[k]
        if q < 2:
            x_of = (1 - at_x) if q == 0 else at_x
            came, kind, index = ya.at[z_of, x_of, strip(0, s)], "fy", z_of * 2 + x_of
        else:
            half = (1 - at_y) if q == 2 else at_y
            came, kind, index = xb.at[z_of, half, strip(0, s)], "fx", z_of * 2 + half
        arrive(came, kind, index * SUB + s)
        add_to(quarter(z_of, q, s), came)

    def second_send(k, s):
        z_of = planes[k]
        for n, to in ((0, "x"), (1, "y")):
            start(None, quarter(z_of, 2 * n, s), fin.at[z_of, n, strip(0, s)], "b" + to, z_of * SUB + s, to)

    def second_sum(k, n, s):
        z_of = planes[k]
        came = fin.at[z_of, n, strip(0, s)]
        arrive(came, "by" if n else "bx", z_of * SUB + s)
        add_to(quarter(z_of, 2 * n + 1, s), came)

    def z_stage(k, q, s):
        z_of = planes[k]
        rises = z_of > at_z
        step = jnp.where(rises, 1, -1)
        side = jnp.where(rises, 0, 1)
        index = (z_of * 4 + q) * SUB + s
        spot = quarter(z_of, q, s)
        came = zin.at[side, z_of, q, strip(0, s)]

        def inbound():
            arrive(came, "s", index)
            add_to(spot, came)

        given(within(at_z - step), inbound)
        names = ["s0" if (kind_of, k) in doubled else "s" for kind_of in (word_for[0] or 1, word_for[0] or 2)]
        chosen = names[0] if names[0] == names[1] else jnp.where(ends, sends[names[0]], sends[names[1]])
        landing = jnp.where((at_z + step == z_of) & (step < 0), slots["t"] - slots["s"] + q * SUB + s, index)
        start(None, spot, came, "s", landing, toward(step), chosen)

    def z_last(q, s):
        for side, condition in ((0, low), (1, high)):
            def inbound(side=side):
                came = zin.at[side, at_z, q, strip(0, s)]
                arrive(came, "t" if side else "s", q * SUB + s + (0 if side else at_z * 4 * SUB))
                add_to(quarter(at_z, q, s), came)

            given(condition, inbound)

    mine = pl.ds(pl.multiple_of((at_z * 4 + 2 * at_x + core) * rows_each, rows_each), rows_each)
    placed = pltpu.make_async_copy(tok, every.at[mine, pl.ds(0, width)], own_sem.at[0])
    placed.start()
    weights = [pltpu.make_async_copy(src, dst, own_sem.at[1 + n])
               for n, (src, dst) in enumerate(((gate_hbm, w_gate), (up_hbm, w_up), (down_hbm, w_down)))]
    picks = [pltpu.make_async_copy(src, dst, own_sem.at[4 + n])
             for n, (src, dst) in enumerate(((ids_hbm, ids), (weight_hbm, weight)))]
    for each in picks:
        each.start()
    greet_all(deep, at_z, devices)
    with jax.named_scope("picks"):
        for each in picks:
            each.wait()
    shape = (wide - width, rows_each)
    lane = lax.broadcasted_iota(jnp.int32, shape, 0)
    named = jnp.where(lane < experts, lane, lane - experts)
    scaled = jnp.zeros(shape, jnp.float32)
    for pick in range(ids.shape[0]):
        scaled = scaled + jnp.where(ids[pick:pick + 1, :] == named, weight[pick:pick + 1, :], 0.0)
    rough = scaled.astype(jnp.bfloat16).astype(jnp.float32)
    every[mine, width:wide] = jnp.where(lane < experts, rough, scaled - rough).T.astype(jnp.bfloat16)
    with jax.named_scope("greet"):
        greet_wait(deep, at_z)
    with jax.named_scope("placed"):
        placed.wait()
    for each in weights:
        each.start()
    for p in range(parts):
        index = at_z * parts + p
        held = block(at_x, core, at_z, p, plane_cols)
        start(high, held, held, "z", index, "up")
        start(low, held, held, "z", index, "down")
        start(None, held, held, "x", index, "x", "x0")
    whole = group_rows(at_x, core, at_z, entire)
    start(None, whole, whole, "c", at_z, "core", "cz0")

    acts = (
        (z_arrives, 2), (x_arrives, 2), (h_arrives, 2), (y_arrives, 3), (complete, 1), (gate_up, 2), (down, 2),
        (halves_meet, 2), (first_sum, 3), (second_send, 2), (z_stage, 3), (second_sum, 3), (z_last, 2),
        (lambda s: second_send(0, s), 1), (lambda n, s: second_sum(0, n, s), 2),
    )
    waited = [False]
    for kind_of in (1, 2):
        found = {(step // 100 % 10, step // 10 % 10) for step in SCHEDULE
                 if step // 1000 % 100 == 10 and step // 100000 in (0, kind_of)}
        both = {k for k, q in found if q == 0}
        stages[kind_of] = (len(both), len({k for k, q in found} - both))
        doubled.update((kind_of, k) for k in both)
    for step in SCHEDULE:
        when, (act, taken) = step // 100000, acts[step // 1000 % 100]
        numbers = (step // 100 % 10, step // 10 % 10, step % 10)[:taken]
        if act is gate_up and not waited[0]:
            waited[0] = True
            with jax.named_scope("weights"):
                for each in weights:
                    each.wait()
        only[0] = (None, ends, inner)[when]
        word_for[0] = when
        with jax.named_scope(str(step)):
            act(*numbers)
    only[0] = None
    out[...] = total[at_z, at_x, at_y]
    def drain(name, ref):
        at = sends[name]
        pltpu.make_async_remote_copy(
            src_ref=ref, dst_ref=ref, send_sem=send.at[at], recv_sem=recv.at[0],
            device_id=devices["x"], device_id_type=MESH).wait_send()

    def some(groups, cols):
        return every.at[pl.ds(0, groups * rows_each), cols]

    with jax.named_scope("drain"):
        for name, groups, cols in (
            ("x0", 1, plane_cols), ("x", deep - 1, x_cols), ("ys", deep - 1, theirs), ("yo", deep, theirs),
            ("cz0", 1, entire), ("cz", deep - 1, plane_cols), ("cx0", 1, plane_cols), ("cx", deep - 1, x_cols),
            ("cys", deep - 1, lacking), ("cyo", deep, lacking),
        ):
            drain(name, some(groups, cols))
        if by_z:
            drain("ch", some(deep - 1, z_cols))
        for name, ref in (("m", total), ("fy", ya), ("fx", xb)):
            drain(name, ref)
        for kind_of, condition in ((1, ends), (2, inner)):
            @pl.when(condition)
            def _(kind_of=kind_of):
                drain("z", some(1 if kind_of == 1 else deep + 1, plane_cols))
                if by_z:
                    drain("h", some(1 if kind_of == 1 else deep + 1, z_cols))
                both, one = stages[kind_of]
                if both:
                    drain("s0", zin.at[0, pl.ds(0, both)])
                if one:
                    drain("s", zin.at[1, pl.ds(0, one), pl.ds(0, 2)])
                for name, n in (("bx", 0), ("by", 1)):
                    drain(name, fin.at[pl.ds(0, one + 1), n])


def local_dense(tokens, expert_ids, route_weight, w_gate, w_up, w_down):
    deep = lax.axis_size("dp")
    rows_each, width = tokens.shape
    hidden_cut = w_gate.shape[2]
    half = width // 2
    wide = width + 128
    plane = PLANE
    by_z = BY_Z
    parts = PARTS
    slab = rows_each // 2
    kind = tokens.dtype
    vmem = pl.BlockSpec(memory_space=pltpu.VMEM)
    hbm = pl.BlockSpec(memory_space=pl.ANY)
    return pl.pallas_call(
        lambda *refs: fused_kernel(deep, plane, by_z, parts, *refs),
        out_shape=jax.ShapeDtypeStruct((rows_each, half), kind),
        in_specs=[hbm] * 6,
        out_specs=vmem,
        scratch_shapes=[
            pltpu.VMEM((deep * 4 * rows_each, wide), kind),
            pltpu.VMEM((width, hidden_cut), kind),
            pltpu.VMEM((width, hidden_cut), kind),
            pltpu.VMEM((hidden_cut, width), kind),
            pltpu.VMEM(expert_ids.shape[::-1], expert_ids.dtype),
            pltpu.VMEM(route_weight.shape[::-1], route_weight.dtype),
            pltpu.VMEM((4 * rows_each, hidden_cut), kind),
            pltpu.VMEM((deep, 4, 2, rows_each, half), kind),
            pltpu.VMEM((deep, 2, 2, rows_each, half), kind),
            pltpu.VMEM((deep, 2, slab, half), kind),
            pltpu.VMEM((deep, 2, slab, half), kind),
            pltpu.VMEM((2, deep, 4, slab, half), kind),
            pltpu.VMEM((deep, 2, slab, half), kind),
            pltpu.SemaphoreType.DMA((6,)),
            pltpu.SemaphoreType.DMA((20,)),
            pltpu.SemaphoreType.DMA((sum(size for _, size in semaphore_slots(deep)),)),
        ],
        compiler_params=pltpu.CompilerParams(
            collective_id=0, has_side_effects=True, vmem_limit_bytes=VMEM_LIMIT),
    )(tokens, expert_ids.T, route_weight.T, w_gate[0], w_up[0], w_down[0])


def solution(mesh):
    dense = mesh.shape["blk"] == 2 and mesh.shape["uly"] == 4 and mesh.shape["dp"] == 4
    return jax.shard_map(
        local_dense if dense else local_slots,
        mesh=mesh,
        in_specs=(
            P(("uly", "dp"), None),
            P(("uly", "dp"), None),
            P(("uly", "dp"), None),
            P(("uly", "dp"), None, "blk"),
            P(("uly", "dp"), None, "blk"),
            P(("uly", "dp"), "blk", None),
        ),
        out_specs=P(("uly", "dp"), "blk"),
        check_vma=False,
    )
```

```python
import jax
import jax.numpy as jnp
from jax import lax
from jax.experimental import pallas as pl
from jax.experimental.pallas import tpu as pltpu
from jax.sharding import PartitionSpec as P


def routing_tables(expert_ids, route_weight, groups, local_count, capacity):
    tokens_here, picks_count = expert_ids.shape
    experts = groups * local_count
    labels = lax.broadcasted_iota(jnp.int32, (1, 1, experts), 2)
    onehot = (expert_ids[:, :, None] == labels).astype(jnp.int32)
    chosen = jnp.sum(onehot, axis=1)
    before = jnp.cumsum(chosen, axis=0) - chosen
    slot_of = jnp.sum(onehot * before[:, None, :], axis=2)
    places = lax.broadcasted_iota(jnp.int32, (1, 1, capacity), 2)
    slot_hot = (slot_of[:, :, None] == places).astype(jnp.float32)
    expert_hot = onehot.astype(jnp.float32).reshape(tokens_here, picks_count, groups, local_count)
    placing = jnp.einsum("tkgl,tkc->gclt", expert_hot, slot_hot)
    placing = placing.reshape(groups * capacity * local_count, tokens_here)
    mixing = jnp.einsum("tkgl,tkc,tk->tgcl", expert_hot, slot_hot, route_weight)
    mixing = mixing.reshape(tokens_here, groups * capacity * local_count)
    return (placing.astype(jnp.bfloat16), mixing)


def local_slots(tokens, expert_ids, route_weight, w_gate, w_up, w_down):
    ulysses_size = lax.axis_size("uly")
    data_size = lax.axis_size("dp")
    cycle_size = lax.axis_size("blk")
    tokens_here, model_width = tokens.shape
    local_count = w_gate.shape[0]
    hidden_cut = w_gate.shape[2]
    groups = ulysses_size * data_size
    experts = groups * local_count
    picks_count = expert_ids.shape[1]
    capacity = min(tokens_here, max(2, 5 * tokens_here * picks_count // (4 * experts)))
    placing, mixing = routing_tables(expert_ids, route_weight, groups, local_count, capacity)
    slice_width = model_width // cycle_size
    rows_total = groups * capacity
    cycle_index = lax.axis_index("blk")
    own_part = lax.dynamic_slice_in_dim(tokens, cycle_index * slice_width, slice_width, 1)
    outgoing = jnp.dot(placing, own_part, preferred_element_type=jnp.float32).astype(jnp.bfloat16)
    outgoing = outgoing.reshape(ulysses_size, data_size, capacity, local_count, slice_width)
    arrived = lax.all_to_all(
        lax.all_to_all(outgoing, "uly", split_axis=0, concat_axis=0, tiled=True),
        "dp",
        split_axis=1,
        concat_axis=1,
        tiled=True,
    )
    arrived = arrived.reshape(rows_total, local_count, slice_width)
    portion = lax.all_gather(arrived, "blk", axis=2, tiled=True)
    gate_more = jnp.einsum("rlw,lwf->rlf", portion, w_gate, preferred_element_type=jnp.float32)
    up_more = jnp.einsum("rlw,lwf->rlf", portion, w_up, preferred_element_type=jnp.float32)
    hidden = (jax.nn.silu(gate_more) * up_more).astype(jnp.bfloat16)
    resplit = lax.all_to_all(w_down, "blk", split_axis=2, concat_axis=1, tiled=True)
    zero_sum = jnp.zeros((slice_width, rows_total * local_count), jnp.float32)
    total = zero_sum
    portion = lax.all_gather(hidden, "blk", axis=2, tiled=True)
    ranges_count = portion.shape[2] // hidden_cut
    for number in range(ranges_count):
        part_hidden = portion[:, :, number * hidden_cut : (number + 1) * hidden_cut]
        part_rows = lax.dynamic_slice_in_dim(resplit, number * hidden_cut, hidden_cut, 1)
        partial_value = jnp.einsum(
            "lfd,rlf->drl", part_rows, part_hidden, preferred_element_type=jnp.float32
        )
        partial_value = partial_value.reshape(slice_width, rows_total * local_count)
        total = total + partial_value.astype(jnp.bfloat16).astype(jnp.float32)
    returned = total.astype(jnp.bfloat16).reshape(
        slice_width, ulysses_size, data_size, capacity, local_count
    )
    returned_rows = lax.all_to_all(
        lax.all_to_all(returned, "uly", split_axis=1, concat_axis=1, tiled=True),
        "dp",
        split_axis=2,
        concat_axis=2,
        tiled=True,
    )
    returned_rows = returned_rows.reshape(slice_width, rows_total * local_count).astype(jnp.float32)
    mixed = lax.dot_general(
        mixing, returned_rows, (((1,), (1,)), ((), ())), precision=lax.Precision.HIGHEST
    )
    return mixed.astype(jnp.bfloat16)


MESH = pl.DeviceIdType.MESH

PLANE, BY_Z, PARTS, SUB = 22 * 128, 2 * 128, 4, 1
VMEM_LIMIT = 54700 << 10


SCHEDULE = (
    200100, 200200, 1000, 100100, 200110, 200210, 201020, 201030, 1010, 101020, 200220, 203101,
    120, 101030, 200130, 200230, 200310, 200300, 202230, 3011, 103012, 100110, 101100, 202200,
    200320, 201220, 202210, 200330, 203103, 3010, 100130, 3102, 1120, 201110, 203012, 201210,
    3013, 100200, 202220, 2100, 100210, 203201, 203300, 203202, 202330, 202310, 203200, 203203,
    201130, 203301, 201100, 203112, 202130, 202300, 4000, 5000, 102130, 103103, 101110, 103100,
    100220, 201230, 5010, 101130, 203212, 6000, 103112, 203113, 202110, 201310, 2120, 103200,
    100230, 103111, 101210, 203110, 202320, 201300, 201200, 6010, 100310, 102110, 103101, 103113,
    101220, 100300, 101200, 103203, 103110, 103201, 100320, 203311, 203213, 203111, 203100, 203210,
    203211, 203303, 201330, 201320, 207000, 4100, 5100, 101230, 100330, 103202, 101310, 207010,
    203310, 5110, 103210, 203302, 203313, 203312, 6100, 101320, 101300, 103302, 6110, 102300,
    102200, 102210, 102220, 102320, 103300, 103212, 101330, 103213, 102310, 102330, 7100, 103311,
    103303, 103310, 102230, 103211, 103301, 107110, 103312, 103313, 4300, 5300, 5310, 108100,
    108120, 109100, 6300, 207110, 6310, 207300, 4200, 5200, 107300, 5210, 108110, 111100,
    110110, 107310, 6200, 108300, 110300, 107200, 207310, 6210, 208000, 207200, 208300, 8320,
    210300, 208120, 10320, 207210, 208030, 208130, 208200, 210200, 8310, 107210, 108200, 208100,
    208110, 208330, 210310, 209100, 8220, 110310, 108330, 108130, 109200, 210220, 10330, 107000,
    8210, 108230, 111110, 111200, 110210, 107010, 111210, 108000, 110230, 112000, 8020, 8010,
    211100, 211110, 210210, 210110, 213000, 208230, 210230, 10130, 108030, 112200, 113000, 212100,
    14000, 112100, 214100, 12300, 114100,
)


def neighbours(deep):
    at_y, at_u, at_z = lax.axis_index("blk"), lax.axis_index("uly"), lax.axis_index("dp")
    at_x, core = at_u // 2, at_u % 2
    devices = {
        "up": {"dp": jnp.minimum(at_z + 1, deep - 1)},
        "down": {"dp": jnp.maximum(at_z - 1, 0)},
        "x": {"uly": (1 - at_x) * 2 + core},
        "y": {"blk": 1 - at_y},
        "core": {"uly": at_x * 2 + 1 - core},
    }
    return at_x, at_y, at_z, core, devices


def greet_all(deep, at_z, devices):
    barrier = pltpu.get_barrier_semaphore()
    for name in ("x", "y", "core"):
        pl.semaphore_signal(barrier, inc=1, device_id=devices[name], device_id_type=MESH)

    @pl.when(at_z > 0)
    def _():
        pl.semaphore_signal(barrier, inc=1, device_id=devices["down"], device_id_type=MESH)

    @pl.when(at_z < deep - 1)
    def _():
        pl.semaphore_signal(barrier, inc=1, device_id=devices["up"], device_id_type=MESH)


def greet_wait(deep, at_z):
    barrier = pltpu.get_barrier_semaphore()
    beside = (at_z > 0).astype(jnp.int32) + (at_z < deep - 1).astype(jnp.int32)
    pl.semaphore_wait(barrier, 3 + beside)


def semaphore_slots(deep):
    pieces, extra = deep * PARTS, deep * PARTS if BY_Z else 0
    return (
        ("z", pieces), ("h", extra), ("x", pieces), ("ys", pieces), ("yo", pieces), ("c", deep), ("m", deep * 2),
        ("fy", deep * 2 * SUB), ("fx", deep * 2 * SUB), ("s", deep * 4 * SUB), ("t", 4 * SUB),
        ("bx", deep * SUB), ("by", deep * SUB),
    )


def orders(deep):
    return [sorted(range(deep), key=lambda p: (abs(p - z), (p < z) == (2 * z < deep))) for z in range(deep)]


def fused_kernel(deep, plane, by_z, parts, tok, ids_hbm, weight_hbm, gate_hbm, up_hbm, down_hbm, out,
                 every, w_gate, w_up, w_down, ids, weight, hidden, part, total, ya, xb, zin, fin, own_sem, send, recv):
    at_x, at_y, at_z, core, devices = neighbours(deep)
    rows_each, width = tok.shape
    wide = every.shape[1]
    half_width = width // 2
    piece = rows_each // parts
    slab = rows_each // 2
    slice_rows = slab // SUB
    apart = wide - plane
    low, high = at_z > 0, at_z < deep - 1
    ends = (at_z == 0) | (at_z == deep - 1)
    inner = (at_z > 0) & (at_z < deep - 1)
    first_cols = at_y * apart
    plane_cols = pl.ds(pl.multiple_of(first_cols, 128), plane)
    theirs = pl.ds(pl.multiple_of(at_y * plane, 128), apart)
    lacking = pl.ds(pl.multiple_of((1 - at_y) * plane, 128), apart)
    x_cols = pl.ds(pl.multiple_of(first_cols + at_y * by_z, 128), plane - by_z)
    z_cols = pl.ds(pl.multiple_of(first_cols + (1 - at_y) * (plane - by_z), 128), max(by_z, 128))
    entire = pl.ds(0, wide)
    arrivals = orders(deep)

    def table(rows, k):
        return sum((at_z == z).astype(jnp.int32) * rows[z][k] for z in range(deep))

    planes = [at_z] + [table(arrivals, k) for k in range(1, deep)]
    pending = []
    only = [None]

    def device(to):
        return devices[to] if isinstance(to, str) else to

    slots, count = {}, 0
    for name, size in semaphore_slots(deep):
        slots[name] = count
        count += size
    names = ("z", "h", "x", "x0", "ys", "yo", "cz", "cz0", "cx", "cx0", "ch", "cys", "cyo", "m", "fy", "fx", "s", "s0", "bx", "by")
    sends = {name: number for number, name in enumerate(names)}

    def copy(src, dst, send_at, recv_at, to):
        return pltpu.make_async_remote_copy(
            src_ref=src, dst_ref=dst, send_sem=send.at[send_at], recv_sem=recv.at[recv_at],
            device_id=device(to), device_id_type=MESH)

    def start(condition, src, dst, kind, index, to, other=None):
        what = (src, dst, other if other is not None and not isinstance(other, str) else sends[other or kind], slots[kind] + index, to)

        def go():
            copy(*what).start()

        if only[0] is not None:
            condition = only[0] if condition is None else only[0] & condition
        if condition is None:
            go()
        else:
            pl.when(condition)(go)
        pending.append((condition, what))

    def do(go):
        if only[0] is None:
            go()
        else:
            pl.when(only[0])(go)

    def given(condition, act):
        before = only[0]
        only[0] = condition if before is None else before & condition
        act()
        only[0] = before

    def arrive(dst, kind, index):
        at = slots[kind] + index
        do(lambda: copy(dst, dst, at, at, "x").wait_recv())

    def group_rows(x_of, core_of, z_of, cols):
        first = (z_of * 4 + 2 * x_of + core_of) * rows_each
        return every.at[pl.ds(pl.multiple_of(first, rows_each), rows_each), cols]

    seen, doubled, stages = {}, set(), {}

    def pass_on(key, held, kind, z_of):
        done = {}
        for kind_of in (1, 2):
            if word_for[0] in (0, kind_of):
                seen[key, kind_of] = seen.get((key, kind_of), 0) + 1
                done[kind_of] = seen[key, kind_of] == parts
        whole = [name for name in done if done[name]]
        if not whole:
            return
        if len(whole) == len(done):
            start(None, held, held, "c", z_of, "core", kind)
        else:
            given(ends if whole[0] == 1 else inner, lambda: start(None, held, held, "c", z_of, "core", kind))

    word_for = [0]

    def block(x_of, core_of, z_of, p, cols):
        first = (z_of * 4 + 2 * x_of + core_of) * rows_each + p * piece
        return every.at[pl.ds(pl.multiple_of(first, piece), piece), cols]

    def from_below(z_of):
        return z_of < at_z

    def toward(step):
        return {"dp": jnp.clip(at_z + step, 0, deep - 1)}

    def within(z_of):
        return (z_of >= 0) & (z_of < deep)

    def z_arrives(k, p):
        z_of = planes[k]
        index = z_of * parts + p
        step = jnp.where(from_below(z_of), 1, -1)
        held = block(at_x, core, z_of, p, plane_cols)
        arrive(held, "z", index)
        start(within(at_z + step), held, held, "z", index, toward(step))
        along = block(at_x, core, z_of, p, x_cols)
        start(None, along, along, "x", index, "x")
        sent = block(at_x, core, z_of, p, theirs)
        start(None, sent, sent, "ys", index, "y")
        pass_on(("z", k), group_rows(at_x, core, z_of, plane_cols), "cz", z_of)

    def x_arrives(k, p):
        z_of = planes[k]
        index = z_of * parts + p
        cols = plane_cols if k == 0 else x_cols
        held = block(1 - at_x, core, z_of, p, cols)
        arrive(held, "x", index)
        sent = block(1 - at_x, core, z_of, p, theirs)
        start(None, sent, sent, "yo", index, "y")
        if k == 0 and by_z:
            extra = block(1 - at_x, core, z_of, p, z_cols)
            start(high, extra, extra, "h", index, "up")
            start(low, extra, extra, "h", index, "down")
        pass_on(("x", k), group_rows(1 - at_x, core, z_of, cols), "cx" if k else "cx0", z_of)

    def h_arrives(k, p):
        z_of = planes[k]
        index = z_of * parts + p
        step = jnp.where(from_below(z_of), 1, -1)
        held = block(1 - at_x, core, z_of, p, z_cols)
        arrive(held, "h", index)
        start(within(at_z + step), held, held, "h", index, toward(step))
        pass_on(("h", k), group_rows(1 - at_x, core, z_of, z_cols), "ch", z_of)

    def y_arrives(k, other, p):
        z_of = planes[k]
        index = z_of * parts + p
        x_of = 1 - at_x if other else at_x
        arrive(block(x_of, core, z_of, p, lacking), "yo" if other else "ys", index)
        pass_on(("y", k, other), group_rows(x_of, core, z_of, lacking), "cyo" if other else "cys", z_of)

    def complete(k):
        arrive(every.at[pl.ds(0, 2 * rows_each), :], "c", planes[k])

    batch = 4 * rows_each
    expert = (2 * at_x + core) * deep + at_z
    experts = 4 * deep

    def gate_up(k, n):
        span = w_gate.shape[1] // 2
        rows = pl.ds(pl.multiple_of(planes[k] * batch, batch), batch)
        cols = pl.ds(n * span, span)
        features = every[rows, 0:width]
        gate = jnp.dot(features, w_gate[:, cols], preferred_element_type=jnp.float32)
        up = jnp.dot(features, w_up[:, cols], preferred_element_type=jnp.float32)
        shares = every[rows, width:wide].astype(jnp.float32)
        lane = lax.broadcasted_iota(jnp.int32, shares.shape, 1)
        mine = (lane == expert) | (lane == expert + experts)
        share = jnp.sum(jnp.where(mine, shares, 0.0), axis=1, keepdims=True)
        hidden[:, cols] = (jax.nn.silu(gate) * up * share).astype(jnp.bfloat16)

    def down(k, n):
        half = (1 - at_y) if n == 0 else at_y
        span = half_width // 2
        z_of = planes[k]

        @pl.loop(0, 2)
        def _(m):
            cols = pl.ds(pl.multiple_of(half * half_width + m * span, span), span)
            value = jnp.dot(hidden[...], w_down[:, cols], preferred_element_type=jnp.float32).astype(jnp.bfloat16)
            into = pl.ds(pl.multiple_of(m * span, span), span)
            for g in range(4):
                part[z_of, g, half, :, into] = value[g * rows_each:(g + 1) * rows_each]

        for x_of in range(2):
            start(None, part.at[z_of, 2 * x_of + 1 - core, half], total.at[z_of, x_of, half],
                  "m", z_of * 2 + half, "core")

    upper, lower = pl.ds(0, slab), pl.ds(slab, slab)

    def added(one, other):
        return (one.astype(jnp.float32) + other.astype(jnp.float32)).astype(jnp.bfloat16)

    def strip(base, s):
        return pl.ds(base + s * slice_rows, slice_rows)

    def halves_meet(k, n):
        half = (1 - at_y) if n == 0 else at_y
        z_of = planes[k]
        arrive(total.at[z_of, :, half], "m", z_of * 2 + half)
        for x_of in (1 - at_x, at_x):
            spot = total.at[z_of, x_of, half]
            add_to(spot, part.at[z_of, 2 * x_of + core, half])
            for s in range(SUB):
                if n == 0:
                    start(None, total.at[z_of, x_of, half, strip(0, s)], ya.at[z_of, x_of, strip(0, s)],
                          "fy", (z_of * 2 + x_of) * SUB + s, "y")
                if x_of is not at_x:
                    start(None, total.at[z_of, x_of, half, strip(slab, s)], xb.at[z_of, half, strip(0, s)],
                          "fx", (z_of * 2 + half) * SUB + s, "x")

    def quarter(z_of, q, s):
        if q < 2:
            return total.at[z_of, (1 - at_x) if q == 0 else at_x, at_y, strip(0, s)]
        return total.at[z_of, at_x, (1 - at_y) if q == 2 else at_y, strip(slab, s)]

    def add_to(spot, other):
        def go():
            spot[...] = added(spot[...], other[...])

        do(go)

    def first_sum(k, q, s):
        z_of = planes[k]
        if q < 2:
            x_of = (1 - at_x) if q == 0 else at_x
            came, kind, index = ya.at[z_of, x_of, strip(0, s)], "fy", z_of * 2 + x_of
        else:
            half = (1 - at_y) if q == 2 else at_y
            came, kind, index = xb.at[z_of, half, strip(0, s)], "fx", z_of * 2 + half
        arrive(came, kind, index * SUB + s)
        add_to(quarter(z_of, q, s), came)

    def second_send(k, s):
        z_of = planes[k]
        for n, to in ((0, "x"), (1, "y")):
            start(None, quarter(z_of, 2 * n, s), fin.at[z_of, n, strip(0, s)], "b" + to, z_of * SUB + s, to)

    def second_sum(k, n, s):
        z_of = planes[k]
        came = fin.at[z_of, n, strip(0, s)]
        arrive(came, "by" if n else "bx", z_of * SUB + s)
        add_to(quarter(z_of, 2 * n + 1, s), came)

    def z_stage(k, q, s):
        z_of = planes[k]
        rises = z_of > at_z
        step = jnp.where(rises, 1, -1)
        side = jnp.where(rises, 0, 1)
        index = (z_of * 4 + q) * SUB + s
        spot = quarter(z_of, q, s)
        came = zin.at[side, z_of, q, strip(0, s)]

        def inbound():
            arrive(came, "s", index)
            add_to(spot, came)

        given(within(at_z - step), inbound)
        names = ["s0" if (kind_of, k) in doubled else "s" for kind_of in (word_for[0] or 1, word_for[0] or 2)]
        chosen = names[0] if names[0] == names[1] else jnp.where(ends, sends[names[0]], sends[names[1]])
        landing = jnp.where((at_z + step == z_of) & (step < 0), slots["t"] - slots["s"] + q * SUB + s, index)
        start(None, spot, came, "s", landing, toward(step), chosen)

    def z_last(q, s):
        for side, condition in ((0, low), (1, high)):
            def inbound(side=side):
                came = zin.at[side, at_z, q, strip(0, s)]
                arrive(came, "t" if side else "s", q * SUB + s + (0 if side else at_z * 4 * SUB))
                add_to(quarter(at_z, q, s), came)

            given(condition, inbound)

    mine = pl.ds(pl.multiple_of((at_z * 4 + 2 * at_x + core) * rows_each, rows_each), rows_each)
    placed = pltpu.make_async_copy(tok, every.at[mine, pl.ds(0, width)], own_sem.at[0])
    placed.start()
    weights = [pltpu.make_async_copy(src, dst, own_sem.at[1 + n])
               for n, (src, dst) in enumerate(((gate_hbm, w_gate), (up_hbm, w_up), (down_hbm, w_down)))]
    picks = [pltpu.make_async_copy(src, dst, own_sem.at[4 + n])
             for n, (src, dst) in enumerate(((ids_hbm, ids), (weight_hbm, weight)))]
    for each in picks:
        each.start()
    greet_all(deep, at_z, devices)
    with jax.named_scope("picks"):
        for each in picks:
            each.wait()
    shape = (wide - width, rows_each)
    lane = lax.broadcasted_iota(jnp.int32, shape, 0)
    named = jnp.where(lane < experts, lane, lane - experts)
    scaled = jnp.zeros(shape, jnp.float32)
    for pick in range(ids.shape[0]):
        scaled = scaled + jnp.where(ids[pick:pick + 1, :] == named, weight[pick:pick + 1, :], 0.0)
    rough = scaled.astype(jnp.bfloat16).astype(jnp.float32)
    every[mine, width:wide] = jnp.where(lane < experts, rough, scaled - rough).T.astype(jnp.bfloat16)
    with jax.named_scope("greet"):
        greet_wait(deep, at_z)
    with jax.named_scope("placed"):
        placed.wait()
    for each in weights:
        each.start()
    for p in range(parts):
        index = at_z * parts + p
        held = block(at_x, core, at_z, p, plane_cols)
        start(high, held, held, "z", index, "up")
        start(low, held, held, "z", index, "down")
        start(None, held, held, "x", index, "x", "x0")
    whole = group_rows(at_x, core, at_z, entire)
    start(None, whole, whole, "c", at_z, "core", "cz0")

    acts = (
        (z_arrives, 2), (x_arrives, 2), (h_arrives, 2), (y_arrives, 3), (complete, 1), (gate_up, 2), (down, 2),
        (halves_meet, 2), (first_sum, 3), (second_send, 2), (z_stage, 3), (second_sum, 3), (z_last, 2),
        (lambda s: second_send(0, s), 1), (lambda n, s: second_sum(0, n, s), 2),
    )
    waited = [False]
    for kind_of in (1, 2):
        found = {(step // 100 % 10, step // 10 % 10) for step in SCHEDULE
                 if step // 1000 % 100 == 10 and step // 100000 in (0, kind_of)}
        both = {k for k, q in found if q == 0}
        stages[kind_of] = (len(both), len({k for k, q in found} - both))
        doubled.update((kind_of, k) for k in both)
    for step in SCHEDULE:
        when, (act, taken) = step // 100000, acts[step // 1000 % 100]
        numbers = (step // 100 % 10, step // 10 % 10, step % 10)[:taken]
        if act is gate_up and not waited[0]:
            waited[0] = True
            with jax.named_scope("weights"):
                for each in weights:
                    each.wait()
        only[0] = (None, ends, inner)[when]
        word_for[0] = when
        with jax.named_scope(str(step)):
            act(*numbers)
    only[0] = None
    out[...] = total[at_z, at_x, at_y]
    def drain(name, ref):
        at = sends[name]
        pltpu.make_async_remote_copy(
            src_ref=ref, dst_ref=ref, send_sem=send.at[at], recv_sem=recv.at[0],
            device_id=devices["x"], device_id_type=MESH).wait_send()

    def some(groups, cols):
        return every.at[pl.ds(0, groups * rows_each), cols]

    with jax.named_scope("drain"):
        for name, groups, cols in (
            ("x0", 1, plane_cols), ("x", deep - 1, x_cols), ("ys", deep - 1, theirs), ("yo", deep, theirs),
            ("cz0", 1, entire), ("cz", deep - 1, plane_cols), ("cx0", 1, plane_cols), ("cx", deep - 1, x_cols),
            ("cys", deep - 1, lacking), ("cyo", deep, lacking),
        ):
            drain(name, some(groups, cols))
        if by_z:
            drain("ch", some(deep - 1, z_cols))
        for name, ref in (("m", total), ("fy", ya), ("fx", xb)):
            drain(name, ref)
        for kind_of, condition in ((1, ends), (2, inner)):
            @pl.when(condition)
            def _(kind_of=kind_of):
                drain("z", some(1 if kind_of == 1 else deep + 1, plane_cols))
                if by_z:
                    drain("h", some(1 if kind_of == 1 else deep + 1, z_cols))
                both, one = stages[kind_of]
                if both:
                    drain("s0", zin.at[0, pl.ds(0, both)])
                if one:
                    drain("s", zin.at[1, pl.ds(0, one), pl.ds(0, 2)])
                for name, n in (("bx", 0), ("by", 1)):
                    drain(name, fin.at[pl.ds(0, one + 1), n])


def local_dense(tokens, expert_ids, route_weight, w_gate, w_up, w_down):
    deep = lax.axis_size("dp")
    rows_each, width = tokens.shape
    hidden_cut = w_gate.shape[2]
    half = width // 2
    wide = width + 128
    plane = PLANE
    by_z = BY_Z
    parts = PARTS
    slab = rows_each // 2
    kind = tokens.dtype
    vmem = pl.BlockSpec(memory_space=pltpu.VMEM)
    hbm = pl.BlockSpec(memory_space=pl.ANY)
    return pl.pallas_call(
        lambda *refs: fused_kernel(deep, plane, by_z, parts, *refs),
        out_shape=jax.ShapeDtypeStruct((rows_each, half), kind),
        in_specs=[hbm] * 6,
        out_specs=vmem,
        scratch_shapes=[
            pltpu.VMEM((deep * 4 * rows_each, wide), kind),
            pltpu.VMEM((width, hidden_cut), kind),
            pltpu.VMEM((width, hidden_cut), kind),
            pltpu.VMEM((hidden_cut, width), kind),
            pltpu.VMEM(expert_ids.shape[::-1], expert_ids.dtype),
            pltpu.VMEM(route_weight.shape[::-1], route_weight.dtype),
            pltpu.VMEM((4 * rows_each, hidden_cut), kind),
            pltpu.VMEM((deep, 4, 2, rows_each, half), kind),
            pltpu.VMEM((deep, 2, 2, rows_each, half), kind),
            pltpu.VMEM((deep, 2, slab, half), kind),
            pltpu.VMEM((deep, 2, slab, half), kind),
            pltpu.VMEM((2, deep, 4, slab, half), kind),
            pltpu.VMEM((deep, 2, slab, half), kind),
            pltpu.SemaphoreType.DMA((6,)),
            pltpu.SemaphoreType.DMA((20,)),
            pltpu.SemaphoreType.DMA((sum(size for _, size in semaphore_slots(deep)),)),
        ],
        compiler_params=pltpu.CompilerParams(
            collective_id=0, has_side_effects=True, vmem_limit_bytes=VMEM_LIMIT),
    )(tokens, expert_ids.T, route_weight.T, w_gate[0], w_up[0], w_down[0])


def solution(mesh):
    dense = mesh.shape["blk"] == 2 and mesh.shape["uly"] == 4 and mesh.shape["dp"] == 4
    return jax.shard_map(
        local_dense if dense else local_slots,
        mesh=mesh,
        in_specs=(
            P(("uly", "dp"), None),
            P(("uly", "dp"), None),
            P(("uly", "dp"), None),
            P(("uly", "dp"), None, "blk"),
            P(("uly", "dp"), None, "blk"),
            P(("uly", "dp"), "blk", None),
        ),
        out_specs=P(("uly", "dp"), "blk"),
        check_vma=False,
    )
```
